32 devices in a mesh: orb: 8 (over y, x, core), walk: 4 (over z).
Axes of the slice: x: 2, y: 2, z: 4, core: 2. Of those that a mesh axis runs over, the one named last changes fastest.
Arguments:
- chol: bfloat16 [32, 2048, 2048], P(None, 'orb', 'walk'), may hold values from -6 to 6
- orbitals: bfloat16 [2048, 1024], replicated, may hold values from -0.125 to 0.125
- greens: bfloat16 [4, 1024, 2048], P('walk'), may hold values from -0.00390625 to 0.00390625
- shift: float32 [32], P('orb'), may hold values from -6 to 6
Outputs:
- force_bias: float32 [4, 32], P('walk', 'orb')
- rotated: bfloat16 [32, 1024, 2048], P('orb', None, 'walk')
The draws below stay inside these ranges and needn't reach their ends.
All inputs are finite; a program needn't handle non-finite values.
Results may differ from the reference program's by a relative error of at most 0.007.
Values may be sent and summed in bfloat16 or wider, within the bound.
A program may use at most 64 MiB of HBM per device.

```python
import jax
import jax.numpy as jnp
from jax import lax

N = 2048
NOCC = 1024
NV = 32
W = 4


def shard_levels(stream_key, shape, pieces, smallest, top_value):
    def one(dim, parts):
        heights = jax.random.uniform(jax.random.fold_in(jax.random.fold_in(stream_key, 6), dim), (parts,), jnp.float32, smallest / len(pieces), top_value / len(pieces))
        return jnp.repeat(jnp.exp(heights), shape[dim] // parts).reshape((-1,) + (1,) * (len(shape) - dim - 1))

    factor_of = one(*pieces[0])
    for cut in pieces[1:]:
        factor_of = factor_of * one(*cut)
    return factor_of


def normal_values(own_key, shape, width, limit, split=(), kind=jnp.bfloat16):
    loudness = shard_levels(own_key, shape, split, -0.22, 0.18) if split else 1.0
    result = jax.random.normal(own_key, shape, jnp.float32) * width * loudness
    return jnp.minimum(jnp.maximum(result, -limit), limit).astype(kind)


def setup_inputs(seed: int = 0) -> dict:
    key_list = jax.random.split(jax.random.key(seed), 5)
    chol = normal_values(key_list[0], (NV, N, N), 1.0, 6.0, ((1, 8), (2, 4)))
    orbitals = normal_values(key_list[1], (N, NOCC), N ** -0.5, 0.125)
    greens = normal_values(key_list[2], (W, NOCC, N), (NOCC * N) ** -0.5, 0.00390625, ((0, 4),))
    shift = normal_values(key_list[3], (NV,), 1.0, 6.0, ((0, 8),), jnp.float32)
    return dict(chol=chol, orbitals=orbitals, greens=greens, shift=shift)


def reference(chol, orbitals, greens, shift):
    flat_greens = greens.reshape(greens.shape[0], -1).astype(jnp.float32)
    orbitals_t = orbitals.T

    def one_vector(matrix):
        rotation = jnp.dot(orbitals_t, matrix, preferred_element_type=jnp.float32)
        column = jnp.dot(flat_greens, rotation.reshape(-1), precision=lax.Precision.HIGHEST)
        return rotation.astype(jnp.bfloat16), column

    rotated, columns = lax.map(one_vector, chol)
    force_bias = columns.T - shift[None, :]
    return (force_bias, rotated)
```

```python
import functools

import jax
import jax.numpy as jnp
from jax import lax
from jax.experimental import pallas as pl
from jax.experimental.pallas import tpu as pltpu
from jax.sharding import PartitionSpec as P

MESH = pl.DeviceIdType.MESH
LANES = 128


def xor(a, b, size):
    total, bit = 0, 1
    while bit < size:
        total = total + ((a // bit + b // bit) % 2) * bit
        bit *= 2
    return total


def kernel(
    n, m, chol, orbitals, greens, shift, bias_out, rotated,
    chunks, chol_v, orb_v, orb_t, greens_v, products, arrived, acc, rounded,
    terms, terms_in, sums, sums_in,
    local_sem, out_sem, send_sem, recv_sem, walk_send, walk_recv,
    term_send, term_recv, sum_send, sum_recv,
):
    me, my_walk = lax.axis_index("orb"), lax.axis_index("walk")
    vectors, rows, cols = chol.shape
    owned = vectors // n
    walkers = greens.shape[0]
    core = me % 2

    loads = [
        pltpu.make_async_copy(greens, greens_v, local_sem.at[0]),
        pltpu.make_async_copy(orbitals, orb_v, local_sem.at[1]),
        pltpu.make_async_copy(chol, chol_v, local_sem.at[2]),
    ]
    for load in loads:
        load.start()

    barrier = pltpu.get_barrier_semaphore()
    for k in range(1, n):
        pl.semaphore_signal(barrier, inc=1, device_id={"orb": xor(me, k, n)}, device_id_type=MESH)
    for k in range(1, m):
        pl.semaphore_signal(
            barrier, inc=1, device_id={"walk": (my_walk + k) % m}, device_id_type=MESH
        )
    pl.semaphore_wait(barrier, n + m - 2)

    def chunk_copy(g, k):
        peer = xor(me, k, n)
        return pltpu.make_async_remote_copy(
            src_ref=chol.at[peer * owned + g],
            dst_ref=chunks.at[k, g],
            send_sem=send_sem.at[k, g],
            recv_sem=recv_sem.at[k, g],
            device_id={"orb": peer},
            device_id_type=MESH,
        )

    def send_vector(g):
        half = n // 2
        for low in range(2):
            if low == 1:
                chunk_copy(g, 1).start()
            for high in range(1, half):
                chip = high + core * (half - 2 * high)
                chunk_copy(g, chip * 2 + low).start()

    early = max(owned - 1, 1)
    for g in range(early):
        send_vector(g)

    loads[0].wait()
    loads[1].wait()
    my_rows = orb_v[pl.ds(pl.multiple_of(me * rows, rows), rows), :]
    for w in range(walkers):
        for j in range(m):
            products[j, w] = jnp.dot(
                my_rows, greens_v[w, :, j * cols : (j + 1) * cols],
                preferred_element_type=jnp.float32,
            ).astype(products.dtype)

    def turn(s, _):
        orb_t[s] = orb_v[pl.ds(pl.multiple_of(s * rows, rows), rows), :].T
        return _

    lax.fori_loop(0, n, turn, 0)

    def walk_copy(k):
        peer = (my_walk + k) % m
        return pltpu.make_async_remote_copy(
            src_ref=products.at[peer],
            dst_ref=arrived.at[m - k],
            send_sem=walk_send.at[k],
            recv_sem=walk_recv.at[m - k],
            device_id={"walk": peer},
            device_id_type=MESH,
        )

    def walk_arrival(k):
        return pltpu.make_async_remote_copy(
            src_ref=products.at[0],
            dst_ref=arrived.at[k],
            send_sem=walk_send.at[k],
            recv_sem=walk_recv.at[k],
            device_id={"walk": (my_walk + k) % m},
            device_id_type=MESH,
        )

    for k in range(1, m):
        walk_copy(k).start()

    loads[2].wait()

    def begin(g, _):
        acc[g] = jnp.dot(orb_t[me], chol_v[me * owned + g], preferred_element_type=jnp.float32)
        return _

    lax.fori_loop(0, owned, begin, 0)
    arrived[0] = products[my_walk]
    for k in range(1, m):
        walk_arrival(k).wait_recv()

    def term(v, _):
        block = chol_v[v].astype(jnp.float32)
        for k in range(m):
            from_walk = (my_walk + k) % m
            for w in range(walkers):
                both = block * arrived[k, w].astype(jnp.float32)
                both = jnp.sum(both, axis=0, keepdims=True)
                part = both[:, :LANES]
                for start in range(LANES, cols, LANES):
                    part = part + both[:, start : start + LANES]
                terms[v // owned, from_walk, w, pl.ds(v % owned, 1), :] = part
        return _

    lax.fori_loop(0, vectors, term, 0)

    def take(g, k):
        chunk_copy(g, k).wait_recv()
        return acc[g] + jnp.dot(
            orb_t[xor(me, k, n)], chunks[k, g], preferred_element_type=jnp.float32
        )

    def add(g):
        def step(k, _):
            acc[g] = take(g, k)
            return _

        return step

    def write(g):
        return pltpu.make_async_copy(rounded.at[g], rotated.at[g], out_sem.at[g])

    def finish(g):
        rounded[g] = take(g, n - 1).astype(rounded.dtype)
        write(g).start()

    def term_copy(k):
        peer = xor(me, k, n)
        return pltpu.make_async_remote_copy(
            src_ref=terms.at[peer],
            dst_ref=terms_in.at[k],
            send_sem=term_send.at[k],
            recv_sem=term_recv.at[k],
            device_id={"orb": peer},
            device_id_type=MESH,
        )

    def sum_copy(k):
        peer = (my_walk + k) % m
        return pltpu.make_async_remote_copy(
            src_ref=sums.at[peer],
            dst_ref=sums_in.at[m - k],
            send_sem=sum_send.at[k],
            recv_sem=sum_recv.at[m - k],
            device_id={"walk": peer},
            device_id_type=MESH,
        )

    def sum_arrival(k):
        return pltpu.make_async_remote_copy(
            src_ref=sums.at[0],
            dst_ref=sums_in.at[k],
            send_sem=sum_send.at[k],
            recv_sem=sum_recv.at[k],
            device_id={"walk": (my_walk + k) % m},
            device_id_type=MESH,
        )

    lax.fori_loop(1, n - 1, add(0), 0)
    for k in range(1, n):
        term_copy(k).start()
    for g in range(early, owned):
        send_vector(g)
    if owned > 1:
        finish(0)

    if owned > 2:
        def vector(g, _):
            lax.fori_loop(1, n - 1, add(g), 0)
            finish(g)
            return _

        lax.fori_loop(1, owned - 1, vector, 0)

    mine = terms[me]
    for k in range(1, n):
        term_copy(k).wait_recv()
        mine = mine + terms_in[k]
    sums[...] = mine
    last = owned - 1
    if owned > 1:
        lax.fori_loop(1, 2, add(last), 0)
    for k in range(1, m):
        sum_copy(k).start()
    if owned > 1:
        lax.fori_loop(2, n - 1, add(last), 0)
    total = sums[my_walk]
    for k in range(1, m):
        sum_arrival(k).wait_recv()
        total = total + sums_in[k]
    bias_out[...] = jnp.sum(total, axis=-1) - shift[...]
    finish(last)

    for k in range(1, m):
        walk_copy(k).wait_send()
        sum_copy(k).wait_send()
    for k in range(1, n):
        term_copy(k).wait_send()

    def drain(g, _):
        def one(k, _):
            chunk_copy(g, k).wait_send()
            return _

        lax.fori_loop(1, n, one, 0)
        write(g).wait()
        return _

    lax.fori_loop(0, owned, drain, 0)


def local(n, m, chol, orbitals, greens, shift):
    vectors, rows, cols = chol.shape
    owned = vectors // n
    walkers, occupied, _ = greens.shape
    bf16, f32 = jnp.bfloat16, jnp.float32
    dma = pltpu.SemaphoreType.DMA
    any_space = pl.BlockSpec(memory_space=pl.ANY)
    vmem = pl.BlockSpec(memory_space=pltpu.VMEM)
    return pl.pallas_call(
        functools.partial(kernel, n, m),
        out_shape=(
            jax.ShapeDtypeStruct((walkers, owned), f32),
            jax.ShapeDtypeStruct((owned, occupied, cols), bf16),
        ),
        in_specs=[any_space, any_space, any_space, vmem],
        out_specs=(vmem, any_space),
        scratch_shapes=[
            pltpu.VMEM((n, owned, rows, cols), bf16),
            pltpu.VMEM(chol.shape, bf16),
            pltpu.VMEM(orbitals.shape, bf16),
            pltpu.VMEM((n, occupied, rows), bf16),
            pltpu.VMEM(greens.shape, bf16),
            pltpu.VMEM((m, walkers, rows, cols), bf16),
            pltpu.VMEM((m, walkers, rows, cols), bf16),
            pltpu.VMEM((owned, occupied, cols), f32),
            pltpu.VMEM((owned, occupied, cols), bf16),
            pltpu.VMEM((n, m, walkers, owned, LANES), f32),
            pltpu.VMEM((n, m, walkers, owned, LANES), f32),
            pltpu.VMEM((m, walkers, owned, LANES), f32),
            pltpu.VMEM((m, walkers, owned, LANES), f32),
            dma((3,)),
            dma((owned,)),
            dma((n, owned)),
            dma((n, owned)),
            dma((m,)),
            dma((m,)),
            dma((n,)),
            dma((n,)),
            dma((m,)),
            dma((m,)),
        ],
        compiler_params=pltpu.CompilerParams(
            collective_id=0, has_side_effects=True, vmem_limit_bytes=60 * 2**20
        ),
    )(chol, orbitals, greens, shift.reshape(1, owned))


def solution(mesh):
    in_specs = (P(None, "orb", "walk"), P(), P("walk", None, None), P("orb"))
    out_specs = (P("walk", "orb"), P("orb", None, "walk"))
    body = functools.partial(local, mesh.shape["orb"], mesh.shape["walk"])
    return jax.shard_map(body, mesh=mesh, in_specs=in_specs, out_specs=out_specs, check_vma=False)
```

```python
import functools

import jax
import jax.numpy as jnp
from jax import lax
from jax.experimental import pallas as pl
from jax.experimental.pallas import tpu as pltpu
from jax.sharding import PartitionSpec as P

MESH = pl.DeviceIdType.MESH
LANES = 128


def xor(a, b, size):
    total, bit = 0, 1
    while bit < size:
        total = total + ((a // bit + b // bit) % 2) * bit
        bit *= 2
    return total


def kernel(
    n, m, chol, orbitals, greens, bias_out, rotated,
    chunks, chol_v, orb_v, orb_t, greens_v, products, arrived, acc,
    terms, terms_in, sums, sums_in,
    local_sem, send_sem, recv_sem, walk_send, walk_recv,
    term_send, term_recv, sum_send, sum_recv,
):
    me, my_walk = lax.axis_index("orb"), lax.axis_index("walk")
    vectors, rows, cols = chol.shape
    owned = vectors // n
    walkers = greens.shape[0]
    core = me % 2

    loads = [
        pltpu.make_async_copy(greens, greens_v, local_sem.at[0]),
        pltpu.make_async_copy(orbitals, orb_v, local_sem.at[1]),
        pltpu.make_async_copy(chol, chol_v, local_sem.at[2]),
    ]

    barrier = pltpu.get_barrier_semaphore()
    for k in range(1, n):
        pl.semaphore_signal(barrier, inc=1, device_id={"orb": xor(me, k, n)}, device_id_type=MESH)
    for k in range(1, m):
        pl.semaphore_signal(
            barrier, inc=1, device_id={"walk": (my_walk + k) % m}, device_id_type=MESH
        )
    pl.semaphore_wait(barrier, n + m - 2)

    def chunk_copy(g, k):
        peer = xor(me, k, n)
        return pltpu.make_async_remote_copy(
            src_ref=chol.at[peer * owned + g],
            dst_ref=chunks.at[k, g],
            send_sem=send_sem.at[k, g],
            recv_sem=recv_sem.at[k, g],
            device_id={"orb": peer},
            device_id_type=MESH,
        )

    def send_vector(g):
        half = n // 2
        for low in range(2):
            if low == 1:
                chunk_copy(g, 1).start()
            for high in range(1, half):
                chip = high + core * (half - 2 * high)
                chunk_copy(g, chip * 2 + low).start()

    early = max(owned - 1, 1)
    for g in range(early):
        send_vector(g)

    for load in loads:
        load.start()
    loads[0].wait()
    loads[1].wait()
    my_rows = orb_v[pl.ds(pl.multiple_of(me * rows, rows), rows), :]
    for w in range(walkers):
        for j in range(m):
            products[j, w] = jnp.dot(
                my_rows, greens_v[w, :, j * cols : (j + 1) * cols],
                preferred_element_type=jnp.float32,
            ).astype(products.dtype)

    def turn(s, _):
        orb_t[s] = orb_v[pl.ds(pl.multiple_of(s * rows, rows), rows), :].T
        return _

    lax.fori_loop(0, n, turn, 0)

    def walk_copy(k):
        peer = (my_walk + k) % m
        return pltpu.make_async_remote_copy(
            src_ref=products.at[peer],
            dst_ref=arrived.at[m - k],
            send_sem=walk_send.at[k],
            recv_sem=walk_recv.at[m - k],
            device_id={"walk": peer},
            device_id_type=MESH,
        )

    def walk_arrival(k):
        return pltpu.make_async_remote_copy(
            src_ref=products.at[0],
            dst_ref=arrived.at[k],
            send_sem=walk_send.at[k],
            recv_sem=walk_recv.at[k],
            device_id={"walk": (my_walk + k) % m},
            device_id_type=MESH,
        )

    for k in range(1, m):
        walk_copy(k).start()

    loads[2].wait()

    def begin(g, _):
        acc[g] = jnp.dot(orb_t[me], chol_v[me * owned + g], preferred_element_type=jnp.float32)
        return _

    lax.fori_loop(0, owned, begin, 0)
    arrived[0] = products[my_walk]
    for k in range(1, m):
        walk_arrival(k).wait_recv()

    def term(v, _):
        block = chol_v[v].astype(jnp.float32)
        for k in range(m):
            from_walk = (my_walk + k) % m
            for w in range(walkers):
                both = block * arrived[k, w].astype(jnp.float32)
                both = jnp.sum(both, axis=0, keepdims=True)
                part = both[:, :LANES]
                for start in range(LANES, cols, LANES):
                    part = part + both[:, start : start + LANES]
                terms[v // owned, from_walk, w, pl.ds(v % owned, 1), :] = part
        return _

    lax.fori_loop(0, vectors, term, 0)

    def take(g, k):
        chunk_copy(g, k).wait_recv()
        return acc[g] + jnp.dot(
            orb_t[xor(me, k, n)], chunks[k, g], preferred_element_type=jnp.float32
        )

    def add(g):
        def step(k, _):
            acc[g] = take(g, k)
            return _

        return step

    def finish(g):
        rotated[g] = take(g, n - 1).astype(rotated.dtype)

    def term_copy(k):
        peer = xor(me, k, n)
        return pltpu.make_async_remote_copy(
            src_ref=terms.at[peer],
            dst_ref=terms_in.at[k],
            send_sem=term_send.at[k],
            recv_sem=term_recv.at[k],
            device_id={"orb": peer},
            device_id_type=MESH,
        )

    def sum_copy(k):
        peer = (my_walk + k) % m
        return pltpu.make_async_remote_copy(
            src_ref=sums.at[peer],
            dst_ref=sums_in.at[m - k],
            send_sem=sum_send.at[k],
            recv_sem=sum_recv.at[m - k],
            device_id={"walk": peer},
            device_id_type=MESH,
        )

    def sum_arrival(k):
        return pltpu.make_async_remote_copy(
            src_ref=sums.at[0],
            dst_ref=sums_in.at[k],
            send_sem=sum_send.at[k],
            recv_sem=sum_recv.at[k],
            device_id={"walk": (my_walk + k) % m},
            device_id_type=MESH,
        )

    lax.fori_loop(1, n - 1, add(0), 0)
    for k in range(1, n):
        term_copy(k).start()
    for g in range(early, owned):
        send_vector(g)
    if owned > 1:
        finish(0)

    if owned > 2:
        def vector(g, _):
            lax.fori_loop(1, n - 1, add(g), 0)
            finish(g)
            return _

        lax.fori_loop(1, owned - 1, vector, 0)

    def drain(g, _):
        def one(k, _):
            chunk_copy(g, k).wait_send()
            return _

        return lax.fori_loop(1, n, one, _)

    last = owned - 1
    lax.fori_loop(0, last, drain, 0)
    for k in range(1, m):
        walk_copy(k).wait_send()
    for k in range(1, n):
        term_copy(k).wait_send()

    mine = terms[me]
    for k in range(1, n):
        term_copy(k).wait_recv()
        mine = mine + terms_in[k]
    sums[...] = mine
    if owned > 1:
        lax.fori_loop(1, 2, add(last), 0)
    for k in range(1, m):
        sum_copy(k).start()
    if owned > 1:
        lax.fori_loop(2, n - 1, add(last), 0)
    total = sums[my_walk]
    for k in range(1, m):
        sum_arrival(k).wait_recv()
        total = total + sums_in[k]
    bias_out[...] = jnp.sum(total, axis=-1)
    finish(last)

    for k in range(1, m):
        sum_copy(k).wait_send()
    drain(last, 0)


def store(bias, shift, rounded, bias_out, rotated, sems):
    writes = [
        pltpu.make_async_copy(rounded.at[g], rotated.at[g], sems.at[g])
        for g in range(rounded.shape[0])
    ]
    for write in writes:
        write.start()
    bias_out[...] = bias[...] - shift[...]
    for write in writes:
        write.wait()


def local(n, m, chol, orbitals, greens, shift):
    vectors, rows, cols = chol.shape
    owned = vectors // n
    walkers, occupied, _ = greens.shape
    bf16, f32 = jnp.bfloat16, jnp.float32
    dma = pltpu.SemaphoreType.DMA
    any_space = pl.BlockSpec(memory_space=pl.ANY)
    vmem = pl.BlockSpec(memory_space=pltpu.VMEM)
    bias, rounded = pl.pallas_call(
        functools.partial(kernel, n, m),
        out_shape=(
            pltpu.VMEM((walkers, owned), f32),
            pltpu.VMEM((owned, occupied, cols), bf16),
        ),
        in_specs=[any_space] * 3,
        out_specs=(vmem, vmem),
        scratch_shapes=[
            pltpu.VMEM((n, owned, rows, cols), bf16),
            pltpu.VMEM(chol.shape, bf16),
            pltpu.VMEM(orbitals.shape, bf16),
            pltpu.VMEM((n, occupied, rows), bf16),
            pltpu.VMEM(greens.shape, bf16),
            pltpu.VMEM((m, walkers, rows, cols), bf16),
            pltpu.VMEM((m, walkers, rows, cols), bf16),
            pltpu.VMEM((owned, occupied, cols), f32),
            pltpu.VMEM((n, m, walkers, owned, LANES), f32),
            pltpu.VMEM((n, m, walkers, owned, LANES), f32),
            pltpu.VMEM((m, walkers, owned, LANES), f32),
            pltpu.VMEM((m, walkers, owned, LANES), f32),
            dma((3,)),
            dma((n, owned)),
            dma((n, owned)),
            dma((m,)),
            dma((m,)),
            dma((n,)),
            dma((n,)),
            dma((m,)),
            dma((m,)),
        ],
        compiler_params=pltpu.CompilerParams(
            collective_id=0, has_side_effects=True, vmem_limit_bytes=59 * 2**20
        ),
    )(chol, orbitals, greens)
    return pl.pallas_call(
        store,
        out_shape=(
            jax.ShapeDtypeStruct((walkers, owned), f32),
            jax.ShapeDtypeStruct((owned, occupied, cols), bf16),
        ),
        in_specs=[vmem, vmem, vmem],
        out_specs=(vmem, any_space),
        scratch_shapes=[dma((owned,))],
        compiler_params=pltpu.CompilerParams(vmem_limit_bytes=2**20),
    )(bias, shift.reshape(1, owned), rounded)


def solution(mesh):
    in_specs = (P(None, "orb", "walk"), P(), P("walk", None, None), P("orb"))
    out_specs = (P("walk", "orb"), P("orb", None, "walk"))
    body = functools.partial(local, mesh.shape["orb"], mesh.shape["walk"])
    return jax.shard_map(body, mesh=mesh, in_specs=in_specs, out_specs=out_specs, check_vma=False)
```
